256 devices in a mesh: copy: 2 (over core), fsdp: 32 (over z, y), tp: 4 (over x).
Axes of the slice: x: 4, y: 4, z: 8, core: 2. Of those that a mesh axis runs over, the one named last changes fastest.
Arguments:
- gradients: float32 [256, 128, 4096], P('copy', 'fsdp', 'tp'), parts along dimension 0, may hold values from -6 to 6
- momentum: float32 [256, 128, 4096], P('copy', 'fsdp', 'tp'), parts along dimension 0, may hold values from -6 to 6
- weights: float32 [256, 128, 4096], P('copy', 'fsdp', 'tp'), parts along dimension 0, may hold values from -0.1875 to 0.1875
Outputs:
- new_weights: float32 [256, 128, 4096], P('copy', 'fsdp', 'tp'), parts along dimension 0
- new_momentum: float32 [256, 128, 4096], P('copy', 'fsdp', 'tp'), parts along dimension 0
The draws below stay inside these ranges and needn't reach their ends.
There are 2 independent parts, one for each index of `copy`. The reference program is written for one: setup_inputs(seed, part) draws one part's arguments, and reference() takes and returns one part's arrays. A program takes and returns all parts, laid end to end along the dimension named above; each array names one. Nothing has to cross between parts.
All inputs are finite; a program needn't handle non-finite values.
Results may differ from the reference program's by a relative error of at most 0.00014.
Values sent between devices are 32-bit elements; how exact they have to be, the bound alone decides.
No kernel may reach another device: no remote copies, remote signals or barrier semaphores. Data moves between devices by JAX's collectives and lax.ppermute only.
A program may use at most 64 MiB of HBM per device.

```python
import jax
import jax.numpy as jnp
from jax import lax

SIDE = 128
WIDE = 4096
MATS = 128
ITERS = 4


def steps_of(stream_key, dims, cuts, low, largest):
    gain, own = 1.0, jax.random.fold_in(stream_key, 6)
    for position, shards_of in cuts:
        steps = jnp.exp(jax.random.uniform(jax.random.fold_in(own, position), (shards_of,), jnp.float32, low / len(cuts), largest / len(cuts)))
        gain = gain * jnp.repeat(steps, dims[position] // shards_of).reshape([-1 if axis == position else 1 for axis in range(len(dims))])
    return gain


def normal_values(key, shape, deviation, reach, shards=(), held_as=jnp.bfloat16):
    factor_of = steps_of(key, shape, shards, -0.22, 0.18) if shards else 1.0
    values = jax.random.normal(key, shape, jnp.float32) * deviation * factor_of
    return jnp.minimum(jnp.maximum(values, -reach), reach).astype(held_as)


def setup_inputs(seed: int = 0, part: int = 0) -> dict:
    arg_keys = jax.random.split(jax.random.key(seed), 4)
    own_keys = jax.random.split(jax.random.fold_in(arg_keys[3], part), 4)
    gradients = normal_values(own_keys[0], (MATS, SIDE, WIDE), 1.0, 6.0, ((1, 32), (2, 4)), jnp.float32)
    momentum = normal_values(own_keys[1], (MATS, SIDE, WIDE), 1.0, 6.0, ((1, 32), (2, 4)), jnp.float32)
    weights = normal_values(own_keys[2], (MATS, SIDE, WIDE), 0.03, 0.1875, ((1, 32), (2, 4)), jnp.float32)
    return dict(gradients=gradients, momentum=momentum, weights=weights)


hold_rate = 0.95
learn_rate = 0.9
decay_rate = 0.1

def reference(gradients, momentum, weights):
    new_momentum = hold_rate * momentum + gradients
    direction = hold_rate * new_momentum + gradients

    def orthogonal_one(stack):
        iterate = stack[None]
        iterate = iterate * lax.rsqrt(lax.optimization_barrier(jnp.sum(iterate * iterate, axis=(1, 2), keepdims=True)) + 1e-06)
        for step in range(ITERS):
            gram = jnp.einsum('mik,mjk->mij', iterate, iterate, precision=lax.Precision.HIGHEST)
            mixed = -4.775 * gram + 2.0315 * jnp.einsum('mij,mjk->mik', gram, gram, precision=lax.Precision.HIGHEST)
            iterate = 3.4445 * iterate + jnp.einsum('mij,mjk->mik', mixed, iterate, precision=lax.Precision.HIGHEST)
        return iterate[0]
    iterate = lax.map(orthogonal_one, direction)
    new_weights = (1.0 - learn_rate * decay_rate) * weights - learn_rate * iterate
    return (new_weights, new_momentum)
```

```python
import jax
import jax.numpy as jnp
from jax import lax
from jax.experimental import pallas as pl
from jax.experimental.pallas import tpu as pltpu
from jax.sharding import PartitionSpec as P

ITERS = 4
hold_rate = 0.95
learn_rate = 0.9
decay_rate = 0.1
LINEAR, CUBIC, QUINTIC = 3.4445, -4.775, 2.0315
OWNERS = ("fsdp", "tp")


def dot(a, b, across=False):
    return lax.dot_general(
        a,
        b,
        (((1,), (1 if across else 0,)), ((), ())),
        precision=lax.Precision.HIGHEST,
        preferred_element_type=jnp.float32,
    )


def whole_matrix(x_ref, y_ref):
    sources, lines, lanes = x_ref.shape
    tps = 4
    fsdps = sources // tps
    pairs = lines // 8
    rows = fsdps * 8
    view = x_ref.reshape(fsdps, tps, lines, lanes)
    out = y_ref.reshape(fsdps, tps, lines, lanes)

    def part(t):
        return jnp.concatenate(
            [view[:, t, p * 8 : p * 8 + 8, :].reshape(rows, lanes) for p in range(pairs)], axis=1
        )

    wide = None
    for t in range(tps):
        z = part(t)
        g = dot(z, z, across=True)
        wide = g if wide is None else wide + g
    i = lax.broadcasted_iota(jnp.int32, (rows, rows), 0)
    j = lax.broadcasted_iota(jnp.int32, (rows, rows), 1)
    same_half = ((i // 4) % 2) == ((j // 4) % 2)
    total = jnp.sum(jnp.sum(jnp.where(i == j, wide, 0.0), axis=1, keepdims=True), axis=0, keepdims=True) + 1e-06
    swapped = jnp.where((i // 4) % 2 == 0, pltpu.roll(wide, rows - 4, 0), pltpu.roll(wide, 4, 0))
    swapped = jnp.where((j // 4) % 2 == 0, pltpu.roll(swapped, rows - 4, 1), pltpu.roll(swapped, 4, 1))
    gram = jnp.where(same_half, (wide + swapped) / total, 0.0)
    applied = None
    for step in range(ITERS):
        extra = (CUBIC / LINEAR) * gram + (QUINTIC / LINEAR) * dot(gram, gram)
        applied = extra if applied is None else applied + (extra + dot(extra, applied))
        if step < ITERS - 1:
            gram = LINEAR**2 * (gram + dot(gram, 2.0 * extra + dot(extra, extra)))
    scale = LINEAR**ITERS * lax.rsqrt(total)
    for t in range(tps):
        z = part(t)
        y = scale * (z + dot(applied, z))
        for p in range(pairs):
            out[:, t, p * 8 : p * 8 + 8, :] = y[:, p * lanes : (p + 1) * lanes].reshape(fsdps, 8, lanes)


def by_tile(x):
    mats, rows, columns = x.shape
    return x.reshape(mats, rows, columns // 128, 128).transpose(0, 2, 1, 3).reshape(mats, rows * columns // 128, 128)


def by_row(x, shape):
    mats, rows, columns = shape
    return x.reshape(mats, columns // 128, rows, 128).transpose(0, 2, 1, 3).reshape(shape)


def shards(gradients, momentum, weights):
    shape = gradients.shape
    gradients_t, momentum_t, weights_t = by_tile(gradients), by_tile(momentum), by_tile(weights)
    new_momentum = hold_rate * momentum_t + gradients_t
    direction = hold_rate * new_momentum + gradients_t
    moved = lax.all_to_all(direction, OWNERS, 0, 0, tiled=True)
    iterate = pl.pallas_call(
        whole_matrix,
        out_shape=jax.ShapeDtypeStruct(moved.shape, jnp.float32),
        in_specs=[pl.BlockSpec(memory_space=pltpu.VMEM)],
        out_specs=pl.BlockSpec(memory_space=pltpu.VMEM),
        cost_estimate=pl.CostEstimate(flops=12 * 1000 * 1000 * 1000, bytes_accessed=4 << 20, transcendentals=0),
        compiler_params=pltpu.CompilerParams(vmem_limit_bytes=40 << 20),
        name="whole_matrix",
    )(moved)
    back = lax.all_to_all(iterate, OWNERS, 0, 0, tiled=True)
    new_weights = (1.0 - learn_rate * decay_rate) * weights_t - learn_rate * back
    return by_row(new_weights, shape), by_row(new_momentum, shape)


def solution(mesh):
    spec = P("copy", "fsdp", "tp")
    return jax.shard_map(
        shards, mesh=mesh, in_specs=(spec, spec, spec), out_specs=(spec, spec), check_vma=False
    )
```

```python
import jax
import jax.numpy as jnp
from jax import lax
from jax.experimental import pallas as pl
from jax.experimental.pallas import tpu as pltpu
from jax.sharding import PartitionSpec as P

ITERS = 4
hold_rate = 0.95
learn_rate = 0.9
decay_rate = 0.1
LINEAR, CUBIC, QUINTIC = 3.4445, -4.775, 2.0315
OWNERS = ("fsdp", "tp")
TURN_NANOS = 22000


def dot(a, b, across=False):
    return lax.dot_general(
        a,
        b,
        (((1,), (1 if across else 0,)), ((), ())),
        precision=lax.Precision.HIGHEST,
        preferred_element_type=jnp.float32,
    )


def whole_matrix(x_ref, y_ref):
    sources, lines, lanes = x_ref.shape
    tps = 4
    fsdps = sources // tps
    pairs = lines // 8
    rows = fsdps * 8
    view = x_ref.reshape(fsdps, tps, lines, lanes)
    out = y_ref.reshape(fsdps, tps, lines, lanes)

    def part(t):
        return jnp.concatenate(
            [view[:, t, p * 8 : p * 8 + 8, :].reshape(rows, lanes) for p in range(pairs)], axis=1
        )

    wide = None
    for t in range(tps):
        z = part(t)
        g = dot(z, z, across=True)
        wide = g if wide is None else wide + g
    i = lax.broadcasted_iota(jnp.int32, (rows, rows), 0)
    j = lax.broadcasted_iota(jnp.int32, (rows, rows), 1)
    same_half = ((i // 4) % 2) == ((j // 4) % 2)
    total = jnp.sum(jnp.sum(jnp.where(i == j, wide, 0.0), axis=1, keepdims=True), axis=0, keepdims=True) + 1e-06
    swapped = jnp.where((i // 4) % 2 == 0, pltpu.roll(wide, rows - 4, 0), pltpu.roll(wide, 4, 0))
    swapped = jnp.where((j // 4) % 2 == 0, pltpu.roll(swapped, rows - 4, 1), pltpu.roll(swapped, 4, 1))
    gram = jnp.where(same_half, (wide + swapped) / total, 0.0)
    applied = None
    for step in range(ITERS):
        extra = (CUBIC / LINEAR) * gram + (QUINTIC / LINEAR) * dot(gram, gram)
        applied = extra if applied is None else applied + (extra + dot(extra, applied))
        if step < ITERS - 1:
            gram = LINEAR**2 * (gram + dot(gram, 2.0 * extra + dot(extra, extra)))
    scale = learn_rate * LINEAR**ITERS * lax.rsqrt(total)
    for t in range(tps):
        z = part(t)
        y = scale * (z + dot(applied, z))
        for p in range(pairs):
            out[:, t, p * 8 : p * 8 + 8, :] = y[:, p * lanes : (p + 1) * lanes].reshape(fsdps, 8, lanes)


def hold(nanos_ref, x_ref, same_ref):
    pl.delay(nanos_ref[0])


def after_turn(x, nanos):
    return pl.pallas_call(
        hold,
        out_shape=jax.ShapeDtypeStruct(x.shape, x.dtype),
        in_specs=[pl.BlockSpec(memory_space=pltpu.SMEM), pl.BlockSpec(memory_space=pl.ANY)],
        out_specs=pl.BlockSpec(memory_space=pl.ANY),
        input_output_aliases={1: 0},
        compiler_params=pltpu.CompilerParams(vmem_limit_bytes=1 << 20),
        name="hold",
    )(((1 - lax.axis_index("copy")) * nanos).reshape(1), x)


def by_tile(x):
    mats, rows, columns = x.shape
    return x.reshape(mats, rows, columns // 128, 128).transpose(0, 2, 1, 3).reshape(mats, rows * columns // 128, 128)


def by_row(x, shape):
    mats, rows, columns = shape
    return x.reshape(mats, columns // 128, rows, 128).transpose(0, 2, 1, 3).reshape(shape)


def shards(gradients, momentum, weights):
    shape = gradients.shape
    direction = by_tile(hold_rate * (hold_rate * momentum + gradients) + gradients)
    direction = after_turn(direction, TURN_NANOS)
    gradients, momentum = lax.optimization_barrier((gradients, momentum))
    new_momentum = hold_rate * momentum + gradients
    moved = lax.all_to_all(direction, OWNERS, 0, 0, tiled=True)
    iterate = pl.pallas_call(
        whole_matrix,
        out_shape=jax.ShapeDtypeStruct(moved.shape, jnp.float32),
        in_specs=[pl.BlockSpec(memory_space=pltpu.VMEM)],
        out_specs=pl.BlockSpec(memory_space=pltpu.VMEM),
        cost_estimate=pl.CostEstimate(flops=12 * 1000 * 1000 * 1000, bytes_accessed=4 << 20, transcendentals=0),
        compiler_params=pltpu.CompilerParams(vmem_limit_bytes=40 << 20),
        name="whole_matrix",
    )(moved)
    back = lax.all_to_all(iterate, OWNERS, 0, 0, tiled=True)
    new_weights = (1.0 - learn_rate * decay_rate) * weights - by_row(back, shape)
    return new_weights, new_momentum


def solution(mesh):
    spec = P("copy", "fsdp", "tp")
    return jax.shard_map(
        shards, mesh=mesh, in_specs=(spec, spec, spec), out_specs=(spec, spec), check_vma=False
    )
```

```python
import jax
import jax.numpy as jnp
from jax import lax
from jax.experimental import pallas as pl
from jax.experimental.pallas import tpu as pltpu
from jax.sharding import PartitionSpec as P

ITERS = 4
hold_rate = 0.95
learn_rate = 0.9
decay_rate = 0.1
LINEAR, CUBIC, QUINTIC = 3.4445, -4.775, 2.0315
OWNERS = ("fsdp", "tp")
TURN_NANOS = 18000


def dot(a, b, across=False):
    return lax.dot_general(
        a, b, (((1,), (1 if across else 0,)), ((), ())), preferred_element_type=jnp.float32
    )


def pieces(x):
    high = x.astype(jnp.bfloat16)
    rest = x - high.astype(jnp.float32)
    middle = rest.astype(jnp.bfloat16)
    return high, middle, (rest - middle.astype(jnp.float32)).astype(jnp.bfloat16)


def left_factors(a):
    high, middle, low = pieces(a)
    first = jnp.concatenate([high, middle], axis=1)
    second = jnp.concatenate([middle, high], axis=1)
    return jnp.concatenate([first, second], axis=0), jnp.concatenate([low, high], axis=1)


def times(factors, high, middle, low):
    main, rest = factors
    rows = rest.shape[0]
    y = dot(main, jnp.concatenate([high, middle], axis=0))
    return (y[:rows] + y[rows:]) + dot(rest, jnp.concatenate([high, low], axis=0))


def product(a, b):
    return times(left_factors(a), *pieces(b))


def whole_matrix(x_ref, y_ref, main_ref, low_ref):
    sources, lines, lanes = x_ref.shape
    rows = low_ref.shape[0]
    tps = sources * 4 // rows
    fsdps = sources // tps
    view = x_ref.reshape(fsdps, tps, lines, lanes)
    out = y_ref.reshape(fsdps, tps, lines, lanes)
    upper = lax.broadcasted_iota(jnp.int32, (fsdps // 2, 8, lanes), 1) < 4
    places = [(t, p, (t * (lines // 8) + p) * 2 * lanes) for t in range(tps) for p in range(lines // 8)]

    def cross(a, b):
        return jnp.where(upper, a, pltpu.roll(b, 4, 1)), jnp.where(upper, pltpu.roll(a, 4, 1), b)

    def columns(t, p):
        z = view[:, t, p * 8 : p * 8 + 8, :].reshape(fsdps // 2, 2, 8, lanes)
        left, right = cross(z[:, 0], z[:, 1])
        return jnp.concatenate([left.reshape(rows, lanes), right.reshape(rows, lanes)], axis=1)

    for t, p, c in places:
        high, middle, low = pieces(columns(t, p))
        main_ref[:rows, c : c + 2 * lanes] = high
        main_ref[rows:, c : c + 2 * lanes] = middle
        low_ref[:, c : c + 2 * lanes] = low
    square = dot(main_ref[...], main_ref[...], across=True)
    mixed = dot(main_ref[:rows], low_ref[...], across=True)
    gram = (
        (square[:rows, :rows] + square[rows:, rows:])
        + (square[:rows, rows:] + square[rows:, :rows])
        + (mixed + mixed.T)
    )
    i = lax.broadcasted_iota(jnp.int32, (rows, rows), 0)
    j = lax.broadcasted_iota(jnp.int32, (rows, rows), 1)
    total = jnp.sum(jnp.sum(jnp.where(i == j, gram, 0.0), axis=1, keepdims=True), axis=0, keepdims=True) + 1e-06
    gram = gram / total
    applied = None
    for step in range(ITERS):
        factors = left_factors(gram)
        extra = (CUBIC / LINEAR) * gram + (QUINTIC / LINEAR) * times(factors, *pieces(gram))
        applied = extra if applied is None else applied + (extra + product(extra, applied))
        if step < ITERS - 1:
            gram = LINEAR**2 * (gram + times(factors, *pieces(2.0 * extra + product(extra, extra))))
    scale = learn_rate * LINEAR**ITERS * lax.rsqrt(total)
    factors = left_factors(applied)
    for t, p, c in places:
        span = slice(c, c + 2 * lanes)
        y = scale * (columns(t, p) + times(factors, main_ref[:rows, span], main_ref[rows:, span], low_ref[:, span]))
        left, right = (y[:, :lanes].reshape(fsdps // 2, 8, lanes), y[:, lanes:].reshape(fsdps // 2, 8, lanes))
        a, b = cross(left, right)
        z = jnp.concatenate([a[:, None], b[:, None]], axis=1).reshape(fsdps, 8, lanes)
        out[:, t, p * 8 : p * 8 + 8, :] = z


CHUNKS = 8


def chunk(c, size):
    return pl.ds(c * (size // CHUNKS), size // CHUNKS)


def stepped(momentum, gradients):
    return hold_rate * momentum + gradients


def first_part(waits_ref, momentum_ref, gradients_ref, direction_ref, new_momentum_ref, m, g, n, reads, writes):
    mats = m.shape[0]

    def read(c, hbm, vmem, k):
        return pltpu.make_async_copy(hbm.at[chunk(c, mats)], vmem.at[chunk(c, mats)], reads.at[k, c])

    def write(c):
        return pltpu.make_async_copy(n.at[chunk(c, mats)], new_momentum_ref.at[chunk(c, mats)], writes.at[c])

    for c in range(CHUNKS):
        read(c, momentum_ref, m, 0).start()
        read(c, gradients_ref, g, 1).start()
    for c in range(CHUNKS):
        read(c, momentum_ref, m, 0).wait()
        read(c, gradients_ref, g, 1).wait()
        at = chunk(c, mats)
        direction_ref[at] = hold_rate * stepped(m[at], g[at]) + g[at]

    @pl.when(waits_ref[0] > 0)
    def _():
        for c in range(CHUNKS):
            at = chunk(c, mats)
            n[at] = stepped(m[at], g[at])
            write(c).start()
        for c in range(CHUNKS):
            write(c).wait()
        pl.delay(waits_ref[0])


def last_part(waits_ref, weights_ref, back_ref, momentum_ref, gradients_ref, kept_ref, new_weights_ref, new_momentum_ref, w, n, writes):
    mats = w.shape[0]

    def write(c, vmem, hbm, k):
        return pltpu.make_async_copy(vmem.at[chunk(c, mats)], hbm.at[chunk(c, mats)], writes.at[k, c])

    for c in range(CHUNKS):
        at = chunk(c, mats)
        w[at] = (1.0 - learn_rate * decay_rate) * weights_ref[at] - back_ref[at]
        write(c, w, new_weights_ref, 0).start()

    @pl.when(waits_ref[0] == 0)
    def _():
        for c in range(CHUNKS):
            at = chunk(c, mats)
            n[at] = stepped(momentum_ref[at], gradients_ref[at])
            write(c, n, new_momentum_ref, 1).start()
        for c in range(CHUNKS):
            write(c, n, new_momentum_ref, 1).wait()

    for c in range(CHUNKS):
        write(c, w, new_weights_ref, 0).wait()


def by_tile(x):
    mats, rows, columns = x.shape
    return x.reshape(mats, rows, columns // 128, 128).transpose(0, 2, 1, 3).reshape(mats, rows * columns // 128, 128)


def by_row(x, shape):
    mats, rows, columns = shape
    return x.reshape(mats, columns // 128, rows, 128).transpose(0, 2, 1, 3).reshape(shape)


def shards(gradients, momentum, weights):
    shape = gradients.shape
    rows = shape[1] * lax.axis_size("fsdp")
    columns = shape[2] * lax.axis_size("tp")
    gradients, momentum, weights = by_tile(gradients), by_tile(momentum), by_tile(weights)
    like = jax.ShapeDtypeStruct(gradients.shape, jnp.float32)
    held = pltpu.VMEM(gradients.shape, jnp.float32)
    in_vmem, in_smem, in_hbm = (pl.BlockSpec(memory_space=m) for m in (pltpu.VMEM, pltpu.SMEM, pltpu.HBM))
    waits = ((1 - lax.axis_index("copy")) * TURN_NANOS).reshape(1)
    direction, new_momentum = pl.pallas_call(
        first_part,
        out_shape=(like, like),
        in_specs=[in_smem, in_hbm, in_hbm],
        out_specs=(in_vmem, in_hbm),
        scratch_shapes=[held, held, held, pltpu.SemaphoreType.DMA((2, CHUNKS)), pltpu.SemaphoreType.DMA((CHUNKS,))],
        compiler_params=pltpu.CompilerParams(vmem_limit_bytes=61 << 20),
        name="first_part",
    )(waits, momentum, gradients)
    moved = lax.all_to_all(direction, OWNERS, 0, 0, tiled=True)
    iterate = pl.pallas_call(
        whole_matrix,
        out_shape=like,
        in_specs=[in_vmem],
        out_specs=in_vmem,
        scratch_shapes=[pltpu.VMEM((2 * rows, columns), jnp.bfloat16), pltpu.VMEM((rows, columns), jnp.bfloat16)],
        cost_estimate=pl.CostEstimate(flops=6 * 1000 * 1000 * 1000, bytes_accessed=4 << 20, transcendentals=0),
        compiler_params=pltpu.CompilerParams(vmem_limit_bytes=24 << 20),
        name="whole_matrix",
    )(moved)
    back = lax.all_to_all(iterate, OWNERS, 0, 0, tiled=True)
    new_weights, new_momentum = pl.pallas_call(
        last_part,
        out_shape=(like, like),
        in_specs=[in_smem, in_vmem, in_vmem, in_vmem, in_vmem, in_hbm],
        out_specs=(in_hbm, in_hbm),
        scratch_shapes=[held, held, pltpu.SemaphoreType.DMA((2, CHUNKS))],
        input_output_aliases={5: 1},
        compiler_params=pltpu.CompilerParams(vmem_limit_bytes=24 << 20),
        name="last_part",
    )(waits, weights, back, momentum, gradients, new_momentum)
    return by_row(new_weights, shape), by_row(new_momentum, shape)


def solution(mesh):
    spec = P("copy", "fsdp", "tp")
    return jax.shard_map(
        shards, mesh=mesh, in_specs=(spec, spec, spec), out_specs=(spec, spec), check_vma=False
    )
```

```python
import jax
import jax.numpy as jnp
from jax import lax
from jax.experimental import pallas as pl
from jax.experimental.pallas import tpu as pltpu
from jax.sharding import PartitionSpec as P

ITERS = 4
hold_rate = 0.95
learn_rate = 0.9
decay_rate = 0.1
LINEAR, CUBIC, QUINTIC = 3.4445, -4.775, 2.0315
OWNERS = ("fsdp", "tp")
TURN_NANOS = 18000


def dot(a, b, across=False):
    return lax.dot_general(
        a, b, (((1,), (1 if across else 0,)), ((), ())), preferred_element_type=jnp.float32
    )


def pieces(x):
    high = x.astype(jnp.bfloat16)
    rest = x - high.astype(jnp.float32)
    middle = rest.astype(jnp.bfloat16)
    return high, middle, (rest - middle.astype(jnp.float32)).astype(jnp.bfloat16)


def left_factors(a):
    high, middle, low = pieces(a)
    first = jnp.concatenate([high, middle], axis=1)
    second = jnp.concatenate([middle, high], axis=1)
    return jnp.concatenate([first, second], axis=0), jnp.concatenate([low, high], axis=1)


def times(factors, high, middle, low):
    main, rest = factors
    rows = rest.shape[0]
    y = dot(main, jnp.concatenate([high, middle], axis=0))
    return (y[:rows] + y[rows:]) + dot(rest, jnp.concatenate([high, low], axis=0))


def product(a, b):
    return times(left_factors(a), *pieces(b))


def whole_matrix(x_ref, y_ref, main_ref, low_ref):
    sources, lines, lanes = x_ref.shape
    rows = low_ref.shape[0]
    tps = sources * 4 // rows
    fsdps = sources // tps
    view = x_ref.reshape(fsdps, tps, lines, lanes)
    out = y_ref.reshape(fsdps, tps, lines, lanes)
    upper = lax.broadcasted_iota(jnp.int32, (fsdps // 2, 8, lanes), 1) < 4
    places = [(t, p, (t * (lines // 8) + p) * 2 * lanes) for t in range(tps) for p in range(lines // 8)]

    def cross(a, b):
        return jnp.where(upper, a, pltpu.roll(b, 4, 1)), jnp.where(upper, pltpu.roll(a, 4, 1), b)

    def columns(t, p):
        z = view[:, t, p * 8 : p * 8 + 8, :].reshape(fsdps // 2, 2, 8, lanes)
        left, right = cross(z[:, 0], z[:, 1])
        return jnp.concatenate([left.reshape(rows, lanes), right.reshape(rows, lanes)], axis=1)

    for t, p, c in places:
        high, middle, low = pieces(columns(t, p))
        main_ref[:rows, c : c + 2 * lanes] = high
        main_ref[rows:, c : c + 2 * lanes] = middle
        low_ref[:, c : c + 2 * lanes] = low
    square = dot(main_ref[...], main_ref[...], across=True)
    mixed = dot(main_ref[:rows], low_ref[...], across=True)
    gram = (
        (square[:rows, :rows] + square[rows:, rows:])
        + (square[:rows, rows:] + square[rows:, :rows])
        + (mixed + mixed.T)
    )
    i = lax.broadcasted_iota(jnp.int32, (rows, rows), 0)
    j = lax.broadcasted_iota(jnp.int32, (rows, rows), 1)
    total = jnp.sum(jnp.sum(jnp.where(i == j, gram, 0.0), axis=1, keepdims=True), axis=0, keepdims=True) + 1e-06
    gram = gram / total
    applied = None
    for step in range(ITERS):
        factors = left_factors(gram)
        extra = (CUBIC / LINEAR) * gram + (QUINTIC / LINEAR) * times(factors, *pieces(gram))
        applied = extra if applied is None else applied + (extra + product(extra, applied))
        if step < ITERS - 1:
            gram = LINEAR**2 * (gram + times(factors, *pieces(2.0 * extra + product(extra, extra))))
    scale = learn_rate * LINEAR**ITERS * lax.rsqrt(total)
    factors = left_factors(applied)
    for t, p, c in places:
        span = slice(c, c + 2 * lanes)
        y = scale * (columns(t, p) + times(factors, main_ref[:rows, span], main_ref[rows:, span], low_ref[:, span]))
        left, right = (y[:, :lanes].reshape(fsdps // 2, 8, lanes), y[:, lanes:].reshape(fsdps // 2, 8, lanes))
        a, b = cross(left, right)
        z = jnp.concatenate([a[:, None], b[:, None]], axis=1).reshape(fsdps, 8, lanes)
        out[:, t, p * 8 : p * 8 + 8, :] = z


CHUNKS = 8


def chunk(c, size):
    return pl.ds(c * (size // CHUNKS), size // CHUNKS)


def stepped(momentum, gradients):
    return hold_rate * momentum + gradients


def first_part(waits_ref, momentum_ref, gradients_ref, direction_ref, new_momentum_ref, m, g, n, reads, writes):
    mats = m.shape[0]

    def read(c, hbm, vmem, k):
        return pltpu.make_async_copy(hbm.at[chunk(c, mats)], vmem.at[chunk(c, mats)], reads.at[k, c])

    def write(c):
        return pltpu.make_async_copy(n.at[chunk(c, mats)], new_momentum_ref.at[chunk(c, mats)], writes.at[c])

    for c in range(CHUNKS):
        read(c, momentum_ref, m, 0).start()
        read(c, gradients_ref, g, 1).start()
    for c in range(CHUNKS):
        read(c, momentum_ref, m, 0).wait()
        read(c, gradients_ref, g, 1).wait()
        at = chunk(c, mats)
        direction_ref[at] = hold_rate * stepped(m[at], g[at]) + g[at]

    @pl.when(waits_ref[0] > 0)
    def _():
        for c in range(CHUNKS):
            at = chunk(c, mats)
            n[at] = stepped(m[at], g[at])
            write(c).start()
        for c in range(CHUNKS):
            write(c).wait()
        pl.delay(waits_ref[0])


def last_part(waits_ref, weights_ref, back_ref, momentum_ref, gradients_ref, kept_ref, new_weights_ref, new_momentum_ref, w, n, writes):
    mats = w.shape[0]

    def write(c, vmem, hbm, k):
        return pltpu.make_async_copy(vmem.at[chunk(c, mats)], hbm.at[chunk(c, mats)], writes.at[k, c])

    for c in range(CHUNKS):
        at = chunk(c, mats)
        w[at] = (1.0 - learn_rate * decay_rate) * weights_ref[at] - back_ref[at]
        write(c, w, new_weights_ref, 0).start()

    @pl.when(waits_ref[0] == 0)
    def _():
        for c in range(CHUNKS):
            at = chunk(c, mats)
            n[at] = stepped(momentum_ref[at], gradients_ref[at])
            write(c, n, new_momentum_ref, 1).start()
        for c in range(CHUNKS):
            write(c, n, new_momentum_ref, 1).wait()

    for c in range(CHUNKS):
        write(c, w, new_weights_ref, 0).wait()


def by_tile(x):
    mats, rows, columns = x.shape
    return x.reshape(mats, rows, columns // 128, 128).transpose(0, 2, 1, 3).reshape(mats, rows * columns // 128, 128)


def by_row(x, shape):
    mats, rows, columns = shape
    return x.reshape(mats, columns // 128, rows, 128).transpose(0, 2, 1, 3).reshape(shape)


def shards(gradients, momentum, weights):
    shape = gradients.shape
    rows = shape[1] * lax.axis_size("fsdp")
    columns = shape[2] * lax.axis_size("tp")
    gradients, momentum, weights = by_tile(gradients), by_tile(momentum), by_tile(weights)
    like = jax.ShapeDtypeStruct(gradients.shape, jnp.float32)
    held = pltpu.VMEM(gradients.shape, jnp.float32)
    in_vmem, in_smem, in_hbm = (pl.BlockSpec(memory_space=m) for m in (pltpu.VMEM, pltpu.SMEM, pltpu.HBM))
    waits = ((1 - lax.axis_index("copy")) * TURN_NANOS).reshape(1)
    direction, new_momentum = pl.pallas_call(
        first_part,
        out_shape=(like, like),
        in_specs=[in_smem, in_hbm, in_hbm],
        out_specs=(in_vmem, in_hbm),
        scratch_shapes=[held, held, held, pltpu.SemaphoreType.DMA((2, CHUNKS)), pltpu.SemaphoreType.DMA((CHUNKS,))],
        compiler_params=pltpu.CompilerParams(vmem_limit_bytes=50 << 20),
        name="first_part",
    )(waits, momentum, gradients)
    moved = lax.all_to_all(direction, OWNERS, 0, 0, tiled=True)
    iterate = pl.pallas_call(
        whole_matrix,
        out_shape=like,
        in_specs=[in_vmem],
        out_specs=in_vmem,
        scratch_shapes=[pltpu.VMEM((2 * rows, columns), jnp.bfloat16), pltpu.VMEM((rows, columns), jnp.bfloat16)],
        cost_estimate=pl.CostEstimate(flops=6 * 1000 * 1000 * 1000, bytes_accessed=4 << 20, transcendentals=0),
        compiler_params=pltpu.CompilerParams(vmem_limit_bytes=24 << 20),
        name="whole_matrix",
    )(moved)
    back = lax.all_to_all(iterate, OWNERS, 0, 0, tiled=True)
    new_weights, new_momentum = pl.pallas_call(
        last_part,
        out_shape=(like, like),
        in_specs=[in_smem, in_vmem, in_vmem, in_vmem, in_vmem, in_hbm],
        out_specs=(in_hbm, in_hbm),
        scratch_shapes=[held, held, pltpu.SemaphoreType.DMA((2, CHUNKS))],
        input_output_aliases={5: 1},
        compiler_params=pltpu.CompilerParams(vmem_limit_bytes=24 << 20),
        name="last_part",
    )(waits, weights, back, momentum, gradients, new_momentum)
    return by_row(new_weights, shape), by_row(new_momentum, shape)


def solution(mesh):
    spec = P("copy", "fsdp", "tp")
    return jax.shard_map(
        shards, mesh=mesh, in_specs=(spec, spec, spec), out_specs=(spec, spec), check_vma=False
    )
```

```python
import jax
import jax.numpy as jnp
from jax import lax
from jax.experimental import pallas as pl
from jax.experimental.pallas import tpu as pltpu
from jax.sharding import PartitionSpec as P

ITERS = 4
hold_rate = 0.95
learn_rate = 0.9
decay_rate = 0.1
LINEAR, CUBIC, QUINTIC = 3.4445, -4.775, 2.0315
OWNERS = ("fsdp", "tp")
TPS, HEIGHT, DEPTH = 4, 8, 4
FAR_FIRST = [z // 2 + HEIGHT // 2 * (z % 2) for z in range(HEIGHT)]
ORDER = [(z * DEPTH + y) * TPS + x for x in range(TPS) for y in range(DEPTH) for z in FAR_FIRST]
PLACES = [sorted((i for i, d in enumerate(ORDER) if d % TPS == t), key=lambda i: ORDER[i]) for t in range(TPS)]
TURN_NANOS = 18000


def dot(a, b, across=False):
    return lax.dot_general(
        a, b, (((1,), (1 if across else 0,)), ((), ())), preferred_element_type=jnp.float32
    )


def pieces(x):
    high = x.astype(jnp.bfloat16)
    rest = x - high.astype(jnp.float32)
    middle = rest.astype(jnp.bfloat16)
    return high, middle, (rest - middle.astype(jnp.float32)).astype(jnp.bfloat16)


def left_factors(a):
    high, middle, low = pieces(a)
    first = jnp.concatenate([high, middle], axis=1)
    second = jnp.concatenate([middle, high], axis=1)
    return jnp.concatenate([first, second], axis=0), jnp.concatenate([low, high], axis=1)


def times(factors, high, middle, low):
    main, rest = factors
    rows = rest.shape[0]
    y = dot(main, jnp.concatenate([high, middle], axis=0))
    return (y[:rows] + y[rows:]) + dot(rest, jnp.concatenate([high, low], axis=0))


def product(a, b):
    (ah, am, al), (bh, bm, bl) = a, b
    side = ah.shape[0]
    upper = jnp.concatenate([bh, bm], axis=0)
    both = dot(jnp.concatenate([ah, am], axis=1), jnp.concatenate([upper, jnp.concatenate([bl, bh], axis=0)], axis=1))
    return both[:, :side] + (both[:, side:] + dot(jnp.concatenate([al, ah], axis=1), upper))


def whole_matrix(x_ref, y_ref, main_ref, low_ref):
    sources, lines, lanes = x_ref.shape
    rows = low_ref.shape[0]
    tps = sources * 4 // rows
    fsdps = sources // tps
    upper = lax.broadcasted_iota(jnp.int32, (fsdps // 2, 8, lanes), 1) < 4
    places = [(t, p, (t * (lines // 8) + p) * 2 * lanes) for t in range(tps) for p in range(lines // 8)]

    def cross(a, b):
        return jnp.where(upper, a, pltpu.roll(b, 4, 1)), jnp.where(upper, pltpu.roll(a, 4, 1), b)

    def columns(t, p):
        a, b = (jnp.stack([x_ref[i, p * 8 : p * 8 + 8, :] for i in PLACES[t][k::2]]) for k in range(2))
        left, right = cross(a, b)
        return jnp.concatenate([left.reshape(rows, lanes), right.reshape(rows, lanes)], axis=1)

    for t, p, c in places:
        high, middle, low = pieces(columns(t, p))
        main_ref[:rows, c : c + 2 * lanes] = high
        main_ref[rows:, c : c + 2 * lanes] = middle
        low_ref[:, c : c + 2 * lanes] = low
    square = dot(main_ref[...], main_ref[...], across=True)
    mixed = dot(main_ref[:rows], low_ref[...], across=True)
    gram = (
        (square[:rows, :rows] + square[rows:, rows:])
        + (square[:rows, rows:] + square[rows:, :rows])
        + (mixed + mixed.T)
    )
    i = lax.broadcasted_iota(jnp.int32, (rows, rows), 0)
    j = lax.broadcasted_iota(jnp.int32, (rows, rows), 1)
    total = jnp.sum(jnp.sum(jnp.where(i == j, gram, 0.0), axis=1, keepdims=True), axis=0, keepdims=True) + 1e-06
    gram = gram / total
    applied = None
    for step in range(ITERS):
        powers = pieces(gram)
        extra = (CUBIC / LINEAR) * gram + (QUINTIC / LINEAR) * product(powers, powers)
        more = pieces(extra)
        if step < ITERS - 1:
            gram = LINEAR**2 * (gram + product(powers, pieces(2.0 * extra + product(more, more))))
        applied = extra if applied is None else applied + (extra + product(more, pieces(applied)))
    scale = learn_rate * LINEAR**ITERS * lax.rsqrt(total)
    factors = left_factors(applied)
    for t, p, c in places:
        span = slice(c, c + 2 * lanes)
        y = scale * (columns(t, p) + times(factors, main_ref[:rows, span], main_ref[rows:, span], low_ref[:, span]))
        left, right = (y[:, :lanes].reshape(fsdps // 2, 8, lanes), y[:, lanes:].reshape(fsdps // 2, 8, lanes))
        a, b = cross(left, right)
        for k, half in enumerate((a, b)):
            for n, i in enumerate(PLACES[t][k::2]):
                y_ref[i, p * 8 : p * 8 + 8, :] = half[n]


CHUNKS = 8


def chunk(c, size):
    return pl.ds(c * (size // CHUNKS), size // CHUNKS)


def stepped(momentum, gradients):
    return hold_rate * momentum + gradients


def first_part(waits_ref, momentum_ref, gradients_ref, direction_ref, new_momentum_ref, m, g, n, reads, writes):
    mats = m.shape[0]

    def read(c, hbm, vmem, k):
        return pltpu.make_async_copy(hbm.at[chunk(c, mats)], vmem.at[chunk(c, mats)], reads.at[k, c])

    def write(c):
        return pltpu.make_async_copy(n.at[chunk(c, mats)], new_momentum_ref.at[chunk(c, mats)], writes.at[c])

    for c in range(CHUNKS):
        read(c, momentum_ref, m, 0).start()
        read(c, gradients_ref, g, 1).start()
    for c in range(CHUNKS):
        read(c, momentum_ref, m, 0).wait()
        read(c, gradients_ref, g, 1).wait()
        at = chunk(c, mats)
        direction_ref[at] = hold_rate * stepped(m[at], g[at]) + g[at]

    @pl.when(waits_ref[0] > 0)
    def _():
        for c in range(CHUNKS):
            at = chunk(c, mats)
            n[at] = stepped(m[at], g[at])
            write(c).start()
        for c in range(CHUNKS):
            write(c).wait()
        pl.delay(waits_ref[0])


def last_part(waits_ref, weights_ref, back_ref, momentum_ref, gradients_ref, kept_ref, new_weights_ref, new_momentum_ref, w, n, writes):
    mats = w.shape[0]

    def write(c, vmem, hbm, k):
        return pltpu.make_async_copy(vmem.at[chunk(c, mats)], hbm.at[chunk(c, mats)], writes.at[k, c])

    for c in range(CHUNKS):
        at = chunk(c, mats)
        w[at] = (1.0 - learn_rate * decay_rate) * weights_ref[at] - back_ref[at]
        write(c, w, new_weights_ref, 0).start()

    @pl.when(waits_ref[0] == 0)
    def _():
        for c in range(CHUNKS):
            at = chunk(c, mats)
            n[at] = stepped(momentum_ref[at], gradients_ref[at])
            write(c, n, new_momentum_ref, 1).start()
        for c in range(CHUNKS):
            write(c, n, new_momentum_ref, 1).wait()

    for c in range(CHUNKS):
        write(c, w, new_weights_ref, 0).wait()


def by_tile(x):
    mats, rows, columns = x.shape
    return x.reshape(mats, rows, columns // 128, 128).transpose(0, 2, 1, 3).reshape(mats, rows * columns // 128, 128)


def by_row(x, shape):
    mats, rows, columns = shape
    return x.reshape(mats, columns // 128, rows, 128).transpose(0, 2, 1, 3).reshape(shape)


def shards(gradients, momentum, weights):
    shape = gradients.shape
    rows = shape[1] * lax.axis_size("fsdp")
    columns = shape[2] * lax.axis_size("tp")
    gradients, momentum, weights = by_tile(gradients), by_tile(momentum), by_tile(weights)
    like = jax.ShapeDtypeStruct(gradients.shape, jnp.float32)
    held = pltpu.VMEM(gradients.shape, jnp.float32)
    in_vmem, in_smem, in_hbm = (pl.BlockSpec(memory_space=m) for m in (pltpu.VMEM, pltpu.SMEM, pltpu.HBM))
    waits = ((1 - lax.axis_index("copy")) * TURN_NANOS).reshape(1)
    direction, new_momentum = pl.pallas_call(
        first_part,
        out_shape=(like, like),
        in_specs=[in_smem, in_hbm, in_hbm],
        out_specs=(in_vmem, in_hbm),
        scratch_shapes=[held, held, held, pltpu.SemaphoreType.DMA((2, CHUNKS)), pltpu.SemaphoreType.DMA((CHUNKS,))],
        compiler_params=pltpu.CompilerParams(vmem_limit_bytes=50 << 20),
        name="first_part",
    )(waits, momentum, gradients)
    moved = lax.all_to_all(direction, OWNERS, 0, 0, tiled=True, axis_index_groups=[ORDER])
    iterate = pl.pallas_call(
        whole_matrix,
        out_shape=like,
        in_specs=[in_vmem],
        out_specs=in_vmem,
        scratch_shapes=[pltpu.VMEM((2 * rows, columns), jnp.bfloat16), pltpu.VMEM((rows, columns), jnp.bfloat16)],
        cost_estimate=pl.CostEstimate(flops=6 * 1000 * 1000 * 1000, bytes_accessed=4 << 20, transcendentals=0),
        compiler_params=pltpu.CompilerParams(vmem_limit_bytes=24 << 20),
        name="whole_matrix",
    )(moved)
    back = lax.all_to_all(iterate, OWNERS, 0, 0, tiled=True, axis_index_groups=[ORDER])
    new_weights, new_momentum = pl.pallas_call(
        last_part,
        out_shape=(like, like),
        in_specs=[in_smem, in_vmem, in_vmem, in_vmem, in_vmem, in_hbm],
        out_specs=(in_hbm, in_hbm),
        scratch_shapes=[held, held, pltpu.SemaphoreType.DMA((2, CHUNKS))],
        input_output_aliases={5: 1},
        compiler_params=pltpu.CompilerParams(vmem_limit_bytes=24 << 20),
        name="last_part",
    )(waits, weights, back, momentum, gradients, new_momentum)
    return by_row(new_weights, shape), by_row(new_momentum, shape)


def solution(mesh):
    spec = P("copy", "fsdp", "tp")
    return jax.shard_map(
        shards, mesh=mesh, in_specs=(spec, spec, spec), out_specs=(spec, spec), check_vma=False
    )
```

```python
import jax
import jax.numpy as jnp
from jax import lax
from jax.experimental import pallas as pl
from jax.experimental.pallas import tpu as pltpu
from jax.sharding import PartitionSpec as P

ITERS = 4
hold_rate = 0.95
learn_rate = 0.9
decay_rate = 0.1
LINEAR, CUBIC, QUINTIC = 3.4445, -4.775, 2.0315
OWNERS = ("fsdp", "tp")
TPS, HEIGHT, DEPTH = 4, 8, 4
FAR_FIRST = [z // 2 + HEIGHT // 2 * (z % 2) for z in range(HEIGHT)]
ORDER = [(z * DEPTH + y) * TPS + x for x in range(TPS) for y in range(DEPTH) for z in FAR_FIRST]
PLACES = [sorted((i for i, d in enumerate(ORDER) if d % TPS == t), key=lambda i: ORDER[i]) for t in range(TPS)]
TURN_NANOS = 18000


def dot(a, b, across=False):
    return lax.dot_general(
        a, b, (((1,), (1 if across else 0,)), ((), ())), preferred_element_type=jnp.float32
    )


def pieces(x):
    high = x.astype(jnp.bfloat16)
    rest = x - high.astype(jnp.float32)
    middle = rest.astype(jnp.bfloat16)
    return high, middle, (rest - middle.astype(jnp.float32)).astype(jnp.bfloat16)


def left_factors(a):
    high, middle, low = pieces(a)
    first = jnp.concatenate([high, middle], axis=1)
    second = jnp.concatenate([middle, high], axis=1)
    return jnp.concatenate([first, second], axis=0), jnp.concatenate([low, high], axis=1)


def times(factors, high, middle, low):
    main, rest = factors
    rows = rest.shape[0]
    y = dot(main, jnp.concatenate([high, middle], axis=0))
    return (y[:rows] + y[rows:]) + dot(rest, jnp.concatenate([high, low], axis=0))


def product(a, b):
    (ah, am, al), (bh, bm, bl) = a, b
    side = ah.shape[0]
    upper = jnp.concatenate([bh, bm], axis=0)
    both = dot(jnp.concatenate([ah, am], axis=1), jnp.concatenate([upper, jnp.concatenate([bl, bh], axis=0)], axis=1))
    return both[:, :side] + (both[:, side:] + dot(jnp.concatenate([al, ah], axis=1), upper))


def whole_matrix(x_ref, y_ref, main_ref, low_ref):
    sources, lines, lanes = x_ref.shape
    rows = low_ref.shape[0]
    tps = sources * 4 // rows
    fsdps = sources // tps
    upper = lax.broadcasted_iota(jnp.int32, (fsdps // 2, 8, lanes), 1) < 4
    places = [(t, p, (t * (lines // 8) + p) * 2 * lanes) for t in range(tps) for p in range(lines // 8)]

    def cross(a, b):
        return jnp.where(upper, a, pltpu.roll(b, 4, 1)), jnp.where(upper, pltpu.roll(a, 4, 1), b)

    def columns(t, p):
        a, b = (jnp.stack([x_ref[i, p * 8 : p * 8 + 8, :] for i in PLACES[t][k::2]]) for k in range(2))
        left, right = cross(a, b)
        return jnp.concatenate([left.reshape(rows, lanes), right.reshape(rows, lanes)], axis=1)

    for t, p, c in places:
        high, middle, low = pieces(columns(t, p))
        main_ref[:rows, c : c + 2 * lanes] = high
        main_ref[rows:, c : c + 2 * lanes] = middle
        low_ref[:, c : c + 2 * lanes] = low
    square = dot(main_ref[...], main_ref[...], across=True)
    mixed = dot(main_ref[:rows], low_ref[...], across=True)
    gram = (
        (square[:rows, :rows] + square[rows:, rows:])
        + (square[:rows, rows:] + square[rows:, :rows])
        + (mixed + mixed.T)
    )
    i = lax.broadcasted_iota(jnp.int32, (rows, rows), 0)
    j = lax.broadcasted_iota(jnp.int32, (rows, rows), 1)
    total = jnp.sum(jnp.sum(jnp.where(i == j, gram, 0.0), axis=1, keepdims=True), axis=0, keepdims=True) + 1e-06
    raw = pieces(gram)
    inverse = 1.0 / total
    square = product(raw, raw) * (inverse * inverse)
    gram = gram * inverse
    applied = None
    for step in range(ITERS):
        powers = pieces(gram)
        extra = (CUBIC / LINEAR) * gram + (QUINTIC / LINEAR) * (square if step == 0 else product(powers, powers))
        more = pieces(extra)
        if step < ITERS - 1:
            gram = LINEAR**2 * (gram + product(powers, pieces(2.0 * extra + product(more, more))))
        applied = extra if applied is None else applied + (extra + product(more, pieces(applied)))
    scale = learn_rate * LINEAR**ITERS * lax.rsqrt(total)
    factors = left_factors(applied)
    for t, p, c in places:
        span = slice(c, c + 2 * lanes)
        y = scale * (columns(t, p) + times(factors, main_ref[:rows, span], main_ref[rows:, span], low_ref[:, span]))
        left, right = (y[:, :lanes].reshape(fsdps // 2, 8, lanes), y[:, lanes:].reshape(fsdps // 2, 8, lanes))
        a, b = cross(left, right)
        for k, half in enumerate((a, b)):
            for n, i in enumerate(PLACES[t][k::2]):
                y_ref[i, p * 8 : p * 8 + 8, :] = half[n]


CHUNKS = 8


def chunk(c, size):
    return pl.ds(c * (size // CHUNKS), size // CHUNKS)


def stepped(momentum, gradients):
    return hold_rate * momentum + gradients


def first_part(waits_ref, momentum_ref, gradients_ref, direction_ref, new_momentum_ref, m, g, n, reads, writes):
    mats = m.shape[0]

    def read(c, hbm, vmem, k):
        return pltpu.make_async_copy(hbm.at[chunk(c, mats)], vmem.at[chunk(c, mats)], reads.at[k, c])

    def write(c):
        return pltpu.make_async_copy(n.at[chunk(c, mats)], new_momentum_ref.at[chunk(c, mats)], writes.at[c])

    for c in range(CHUNKS):
        read(c, momentum_ref, m, 0).start()
        read(c, gradients_ref, g, 1).start()
    for c in range(CHUNKS):
        read(c, momentum_ref, m, 0).wait()
        read(c, gradients_ref, g, 1).wait()
        at = chunk(c, mats)
        direction_ref[at] = hold_rate * stepped(m[at], g[at]) + g[at]

    @pl.when(waits_ref[0] > 0)
    def _():
        for c in range(CHUNKS):
            at = chunk(c, mats)
            n[at] = stepped(m[at], g[at])
            write(c).start()
        for c in range(CHUNKS):
            write(c).wait()
        pl.delay(waits_ref[0])


def last_part(waits_ref, weights_ref, back_ref, momentum_ref, gradients_ref, kept_ref, new_weights_ref, new_momentum_ref, w, n, writes):
    mats = w.shape[0]

    def write(c, vmem, hbm, k):
        return pltpu.make_async_copy(vmem.at[chunk(c, mats)], hbm.at[chunk(c, mats)], writes.at[k, c])

    for c in range(CHUNKS):
        at = chunk(c, mats)
        w[at] = (1.0 - learn_rate * decay_rate) * weights_ref[at] - back_ref[at]
        write(c, w, new_weights_ref, 0).start()

    @pl.when(waits_ref[0] == 0)
    def _():
        for c in range(CHUNKS):
            at = chunk(c, mats)
            n[at] = stepped(momentum_ref[at], gradients_ref[at])
            write(c, n, new_momentum_ref, 1).start()
        for c in range(CHUNKS):
            write(c, n, new_momentum_ref, 1).wait()

    for c in range(CHUNKS):
        write(c, w, new_weights_ref, 0).wait()


def by_tile(x):
    mats, rows, columns = x.shape
    return x.reshape(mats, rows, columns // 128, 128).transpose(0, 2, 1, 3).reshape(mats, rows * columns // 128, 128)


def by_row(x, shape):
    mats, rows, columns = shape
    return x.reshape(mats, columns // 128, rows, 128).transpose(0, 2, 1, 3).reshape(shape)


def shards(gradients, momentum, weights):
    shape = gradients.shape
    rows = shape[1] * lax.axis_size("fsdp")
    columns = shape[2] * lax.axis_size("tp")
    gradients, momentum, weights = by_tile(gradients), by_tile(momentum), by_tile(weights)
    like = jax.ShapeDtypeStruct(gradients.shape, jnp.float32)
    held = pltpu.VMEM(gradients.shape, jnp.float32)
    in_vmem, in_smem, in_hbm = (pl.BlockSpec(memory_space=m) for m in (pltpu.VMEM, pltpu.SMEM, pltpu.HBM))
    waits = ((1 - lax.axis_index("copy")) * TURN_NANOS).reshape(1)
    direction, new_momentum = pl.pallas_call(
        first_part,
        out_shape=(like, like),
        in_specs=[in_smem, in_hbm, in_hbm],
        out_specs=(in_vmem, in_hbm),
        scratch_shapes=[held, held, held, pltpu.SemaphoreType.DMA((2, CHUNKS)), pltpu.SemaphoreType.DMA((CHUNKS,))],
        compiler_params=pltpu.CompilerParams(vmem_limit_bytes=50 << 20),
        name="first_part",
    )(waits, momentum, gradients)
    moved = lax.all_to_all(direction, OWNERS, 0, 0, tiled=True, axis_index_groups=[ORDER])
    iterate = pl.pallas_call(
        whole_matrix,
        out_shape=like,
        in_specs=[in_vmem],
        out_specs=in_vmem,
        scratch_shapes=[pltpu.VMEM((2 * rows, columns), jnp.bfloat16), pltpu.VMEM((rows, columns), jnp.bfloat16)],
        cost_estimate=pl.CostEstimate(flops=6 * 1000 * 1000 * 1000, bytes_accessed=4 << 20, transcendentals=0),
        compiler_params=pltpu.CompilerParams(vmem_limit_bytes=24 << 20),
        name="whole_matrix",
    )(moved)
    back = lax.all_to_all(iterate, OWNERS, 0, 0, tiled=True, axis_index_groups=[ORDER])
    new_weights, new_momentum = pl.pallas_call(
        last_part,
        out_shape=(like, like),
        in_specs=[in_smem, in_vmem, in_vmem, in_vmem, in_vmem, in_hbm],
        out_specs=(in_hbm, in_hbm),
        scratch_shapes=[held, held, pltpu.SemaphoreType.DMA((2, CHUNKS))],
        input_output_aliases={5: 1},
        compiler_params=pltpu.CompilerParams(vmem_limit_bytes=24 << 20),
        name="last_part",
    )(waits, weights, back, momentum, gradients, new_momentum)
    return by_row(new_weights, shape), by_row(new_momentum, shape)


def solution(mesh):
    spec = P("copy", "fsdp", "tp")
    return jax.shard_map(
        shards, mesh=mesh, in_specs=(spec, spec, spec), out_specs=(spec, spec), check_vma=False
    )
```
